32 devices in a mesh: layer: 8 (over y, x, core), latent: 4 (over z).
Axes of the slice: x: 2, y: 2, z: 4, core: 2. Of those that a mesh axis runs over, the one named last changes fastest.
Arguments:
- decoder: bfloat16 [65536, 4, 2304], P(('layer', 'latent')), may hold values from -0.375 to 0.375
- code_index: int32 [4, 128, 64], replicated, may hold values from 0 to 16383, all different within a row
- code_value: bfloat16 [4, 128, 64], replicated, may hold values from 0.19921875 to 4
- bias: float32 [4, 2304], replicated, may hold values from -3 to 3
- target: bfloat16 [4, 128, 2304], replicated, may hold values from -6 to 6
Outputs:
- layer_error: float32 [4], replicated
- grad_decoder: bfloat16 [65536, 4, 2304], P(('layer', 'latent'))
- code_grad: float32 [4, 128, 64], replicated
The draws below stay inside these ranges and needn't reach their ends.
Inputs may be any that keep to these rules, and one draw needn't show every extreme that they name: `code_index`: the 64 indices of one token in one layer are distinct.
All inputs are finite; a program needn't handle non-finite values.
Results may differ from the reference program's by a relative error of at most 0.0048.
Values may be sent and summed in bfloat16 or wider, within the bound.
No kernel may reach another device: no remote copies, remote signals or barrier semaphores. Data moves between devices by JAX's collectives and lax.ppermute only.
A program may use at most 192 MiB of HBM per device.

```python
import math
import jax
import jax.numpy as jnp
from jax import lax

D = 2304
F = 16384
LAYERS = 4
TOPK = 64
TOKENS = 128


def shard_levels(own_key, shape, pieces, low, high):
    factor_of = 1.0
    for dim, shards_of in pieces:
        steps = jax.random.uniform(jax.random.fold_in(jax.random.fold_in(own_key, 6), dim), (shards_of,), jnp.float32, low / len(pieces), high / len(pieces))
        factor_of = factor_of * jnp.repeat(jnp.exp(steps), shape[dim] // shards_of).reshape((-1,) + (1,) * (len(shape) - 1 - dim))
    return factor_of


def choose_distinct(key, rows, count, top, lift):
    order = jax.random.permutation(jax.random.fold_in(key, 1), count)
    boost = order
    for power in range(3):
        boost = boost * boost // count
    boost = boost * lift // count
    lots = jax.random.randint(jax.random.fold_in(key, 2), (rows, count), 0, 4096) + boost
    sure = jax.random.permutation(jax.random.fold_in(key, 3), rows)[jnp.arange(count) % rows]
    lots = jnp.where(jnp.arange(rows)[:, None] == sure[None, :], 1 << 14, lots)
    merit = lots * count + jnp.arange(count)
    return lax.top_k(merit.astype(jnp.int32), top)[1].astype(jnp.int32)


def normal_values(key, extent, deviation, limit, pieces=(), held_as=jnp.bfloat16):
    drawn = jax.random.normal(key, extent, jnp.float32) * deviation
    if len(pieces) > 0:
        drawn = shard_levels(key, extent, pieces, -0.22, 0.18) * drawn
    return jnp.clip(drawn, min=-limit, max=limit).astype(held_as)


def setup_inputs(seed: int = 0) -> dict:
    key_of = jax.random.split(jax.random.key(seed), 6)
    decoder = normal_values(key_of[0], (LAYERS * F, LAYERS, D), (LAYERS * TOPK) ** -0.5, 0.375, ((0, 32),))
    code_index = choose_distinct(key_of[1], LAYERS * TOKENS, F, TOPK, 32).reshape((LAYERS, TOKENS, TOPK))
    code_value = jnp.clip(jnp.exp(jax.random.uniform(key_of[2], (LAYERS, TOKENS, TOPK), jnp.float32, math.log(0.19921875), math.log(4.0))), 0.19921875, 4.0).astype(jnp.bfloat16)
    bias = normal_values(key_of[3], (LAYERS, D), 0.5, 3.0, (), jnp.float32)
    target = normal_values(key_of[4], (LAYERS, TOKENS, D), 1.0, 6.0)
    return {"decoder": decoder, "code_index": code_index, "code_value": code_value, "bias": bias, "target": target}


def reference(decoder, code_index, code_value, bias, target):
    token_count = code_index.shape[1]
    token_rows = jnp.arange(token_count, dtype=jnp.int32)[:, None]
    dense_codes = []
    for src_layer in range(LAYERS):
        filled = jnp.zeros((token_count, F), jnp.float32).at[token_rows, code_index[src_layer]].add(code_value[src_layer].astype(jnp.float32))
        dense_codes.append(filled.astype(jnp.bfloat16))
    errors = []
    for tgt_layer in range(LAYERS):
        recon_sum = jnp.zeros((token_count, D), jnp.float32)
        for src_layer in range(tgt_layer + 1):
            weight_slab = decoder[src_layer * F:(src_layer + 1) * F, tgt_layer, :]
            recon_sum = recon_sum + jnp.dot(dense_codes[src_layer], weight_slab, preferred_element_type=jnp.float32)
        errors.append(recon_sum + bias[tgt_layer][None, :] - target[tgt_layer].astype(jnp.float32))
    residual = jnp.stack(errors)
    layer_error = jnp.mean(residual * residual, axis=(1, 2))
    error_b = residual.astype(jnp.bfloat16)
    grad_rows = []
    code_grads = []
    for src_layer in range(LAYERS):
        blocks = []
        code_sums = jnp.zeros((token_count, F), jnp.float32)
        for tgt_layer in range(LAYERS):
            if tgt_layer < src_layer:
                blocks.append(jnp.zeros((F, D), jnp.bfloat16))
            else:
                weight_slab = decoder[src_layer * F:(src_layer + 1) * F, tgt_layer, :]
                blocks.append(jnp.dot(dense_codes[src_layer].T, error_b[tgt_layer], preferred_element_type=jnp.float32).astype(jnp.bfloat16))
                code_sums = code_sums + jnp.dot(error_b[tgt_layer], weight_slab.T, preferred_element_type=jnp.float32)
        grad_rows.append(jnp.stack(blocks, axis=1))
        code_grads.append(jnp.take_along_axis(code_sums, code_index[src_layer], axis=1))
    return layer_error, jnp.concatenate(grad_rows, axis=0), jnp.stack(code_grads)
```

```python
import functools

import jax
import jax.numpy as jnp
from jax import lax
from jax.experimental import pallas as pl
from jax.experimental.pallas import tpu as pltpu
from jax.sharding import Mesh, PartitionSpec as P


LAYERS = 4
UNROLL = 4
RING = 64
LEAD = RING - 2
LANES = 128
VMEM_LIMIT = 56 * 2**20


def advance(groups_ref, tokens, n, g):
    last = g + 1 >= groups_ref[n]
    return jnp.where(last, jnp.minimum(n + 1, tokens - 1), n), jnp.where(last, 0, g + 1)


def load_tables(meta_ref, pairs, sem):
    rows = pairs[0][0].shape[0]
    head = min(16, rows)
    for src, dst in pairs:
        pltpu.make_async_copy(src.at[pl.ds(0, head)], dst.at[pl.ds(0, head)], sem).start()
    for src, dst in pairs:
        pltpu.make_async_copy(src.at[pl.ds(0, head)], dst.at[pl.ds(0, head)], sem).wait()
    if rows > head:
        @pl.when(meta_ref[1] > head)
        def _():
            for src, dst in pairs:
                copy = pltpu.make_async_copy(
                    src.at[pl.ds(head, rows - head)], dst.at[pl.ds(head, rows - head)], sem)
                copy.start()
                copy.wait()


def gather_loop(meta_ref, groups_ref, lat_ref, dec_ref, buf, sems, body, init):
    tokens = groups_ref.shape[0]
    total = meta_ref[0]

    def issue(i, n, g):
        slot = lax.rem(i, RING)
        for u in range(UNROLL):
            row = lat_ref[g * UNROLL + u, n]
            pltpu.make_async_copy(dec_ref.at[row], buf.at[slot * UNROLL + u], sems.at[slot]).start()

    def fill(i, state):
        issue(i, *state)
        return advance(groups_ref, tokens, *state)

    zero = jnp.int32(0)
    ahead = lax.fori_loop(0, jnp.minimum(total, LEAD), fill, (zero, zero))

    def step(i, state):
        ahead_n, ahead_g, n, g, carry = state

        @pl.when(i + LEAD < total)
        def _():
            issue(i + LEAD, ahead_n, ahead_g)

        ahead_n, ahead_g = advance(groups_ref, tokens, ahead_n, ahead_g)
        slot = lax.rem(i, RING)
        pltpu.make_async_copy(
            dec_ref.at[pl.ds(0, UNROLL)], buf.at[pl.ds(slot * UNROLL, UNROLL)], sems.at[slot]).wait()
        carry = body(n, g, slot, carry)
        n, g = advance(groups_ref, tokens, n, g)
        return ahead_n, ahead_g, n, g, carry

    lax.fori_loop(0, total, step, (*ahead, zero, zero, init))


def forward_kernel(meta_ref, groups_ref, lat_hbm, val_hbm, dec_ref, out_ref,
                   lat_ref, val_ref, buf, mixed, table_sem, sems):
    targets, tokens, width = out_ref.shape
    load_tables(meta_ref, ((lat_hbm, lat_ref), (val_hbm, val_ref)), table_sem)

    def body(n, g, slot, total):
        total = jnp.where(g == 0, 0.0, total)
        for u in range(UNROLL):
            total = total + buf[slot * UNROLL + u].astype(jnp.float32) * val_ref[g * UNROLL + u, n]
        for d in range(width // LANES):
            mixed[d, pl.ds(n * targets, targets), :] = total[:, d * LANES:(d + 1) * LANES]
        return total

    gather_loop(meta_ref, groups_ref, lat_ref, dec_ref, buf, sems, body,
                jnp.zeros((targets, width), jnp.float32))
    for d in range(width // LANES):
        for t in range(targets):
            out_ref[t, :, d * LANES:(d + 1) * LANES] = mixed[d, pl.ds(t, tokens, stride=targets), :]


def code_grad_kernel(meta_ref, groups_ref, lat_hbm, err_ref, dec_ref, out_ref,
                     lat_ref, buf, mixed, err_rows, table_sem, sems):
    targets, tokens, width = err_ref.shape
    load_tables(meta_ref, ((lat_hbm, lat_ref),), table_sem)
    out_ref[...] = jnp.zeros_like(out_ref)
    for d in range(width // LANES):
        for t in range(targets):
            mixed[d, pl.ds(t, tokens, stride=targets), :] = (
                err_ref[t, :, d * LANES:(d + 1) * LANES].astype(jnp.float32))

    def spread(n, _):
        for d in range(width // LANES):
            err_rows[n, :, d * LANES:(d + 1) * LANES] = mixed[d, pl.ds(n * targets, targets), :]
        return 0

    lax.fori_loop(0, tokens, spread, 0)
    lane = lax.broadcasted_iota(jnp.int32, (UNROLL, tokens), 1)
    sub = lax.broadcasted_iota(jnp.int32, (UNROLL, tokens), 0)

    def body(n, g, slot, carry):
        err = err_rows[n]
        column = jnp.zeros((UNROLL, tokens), jnp.float32)
        for u in range(UNROLL):
            product = buf[slot * UNROLL + u].astype(jnp.float32) * err
            folded = product[:, :LANES]
            for d in range(1, width // LANES):
                folded = folded + product[:, d * LANES:(d + 1) * LANES]
            column = jnp.where(sub == u, jnp.sum(folded, axis=(0, 1), keepdims=True), column)
        rows = pl.ds(pl.multiple_of(g * UNROLL, UNROLL), UNROLL)
        out_ref[rows, :] = jnp.where(lane == n, column, out_ref[rows, :])
        return carry

    gather_loop(meta_ref, groups_ref, lat_ref, dec_ref, buf, sems, body, jnp.int32(0))


def grad_kernel(codes_ref, err_ref, out_ref, mixed):
    targets, tokens, width = err_ref.shape
    block = out_ref.shape[0]
    codes = codes_ref[...]
    wide = 2 * LANES
    for t in range(targets):
        for d in range(width // wide):
            part = jnp.dot(codes, err_ref[t, :, d * wide:(d + 1) * wide],
                           preferred_element_type=jnp.float32)
            for h in range(2):
                mixed[2 * d + h, pl.ds(t, block, stride=targets), :] = part[:, h * LANES:(h + 1) * LANES]
    for d in range(width // LANES):
        out_ref[:, :, d * LANES:(d + 1) * LANES] = (
            mixed[d].reshape(block, targets, LANES).astype(out_ref.dtype))


def smem():
    return pl.BlockSpec(memory_space=pltpu.SMEM)


def anywhere():
    return pl.BlockSpec(memory_space=pl.ANY)


def vmem():
    return pl.BlockSpec(memory_space=pltpu.VMEM)


def gather_scratch(targets, width):
    return [pltpu.VMEM((RING * UNROLL, targets, width), jnp.bfloat16)]


def partial_recon(meta, groups, lat, val, decoder, tokens):
    _, targets, width = decoder.shape
    return pl.pallas_call(
        forward_kernel,
        out_shape=jax.ShapeDtypeStruct((targets, tokens, width), jnp.float32),
        in_specs=[smem(), smem(), anywhere(), anywhere(), anywhere()],
        out_specs=vmem(),
        scratch_shapes=[
            pltpu.SMEM(lat.shape, jnp.int32),
            pltpu.SMEM(val.shape, jnp.float32),
            *gather_scratch(targets, width),
            pltpu.VMEM((width // LANES, tokens * targets, LANES), jnp.float32),
            pltpu.SemaphoreType.DMA,
            pltpu.SemaphoreType.DMA((RING,)),
        ],
        compiler_params=pltpu.CompilerParams(vmem_limit_bytes=VMEM_LIMIT),
        cost_estimate=pl.CostEstimate(flops=2 * 10**10, bytes_accessed=25 * 10**6, transcendentals=0),
        name="partial_recon",
    )(meta, groups, lat, val, decoder)


def picked_grads(meta, groups, lat, err, decoder):
    targets, tokens, width = err.shape
    return pl.pallas_call(
        code_grad_kernel,
        out_shape=jax.ShapeDtypeStruct((lat.shape[0], tokens), jnp.float32),
        in_specs=[smem(), smem(), anywhere(), vmem(), anywhere()],
        out_specs=vmem(),
        scratch_shapes=[
            pltpu.SMEM(lat.shape, jnp.int32),
            *gather_scratch(targets, width),
            pltpu.VMEM((width // LANES, tokens * targets, LANES), jnp.float32),
            pltpu.VMEM((tokens, targets, width), jnp.float32),
            pltpu.SemaphoreType.DMA,
            pltpu.SemaphoreType.DMA((RING,)),
        ],
        compiler_params=pltpu.CompilerParams(vmem_limit_bytes=VMEM_LIMIT),
        cost_estimate=pl.CostEstimate(flops=2 * 10**10, bytes_accessed=25 * 10**6, transcendentals=0),
        name="picked_grads",
    )(meta, groups, lat, err, decoder)


def decoder_grads(codes_t, err, block):
    slab, tokens = codes_t.shape
    targets, _, width = err.shape
    return pl.pallas_call(
        grad_kernel,
        grid=(slab // block,),
        out_shape=jax.ShapeDtypeStruct((slab, targets, width), jnp.bfloat16),
        in_specs=[
            pl.BlockSpec((block, tokens), lambda i: (i, 0)),
            pl.BlockSpec((targets, tokens, width), lambda i: (0, 0, 0)),
        ],
        out_specs=pl.BlockSpec((block, targets, width), lambda i: (i, 0, 0)),
        scratch_shapes=[pltpu.VMEM((width // LANES, block * targets, LANES), jnp.float32)],
        compiler_params=pltpu.CompilerParams(vmem_limit_bytes=VMEM_LIMIT),
        cost_estimate=pl.CostEstimate(flops=3 * 10**10, bytes_accessed=40 * 10**6, transcendentals=0),
        name="decoder_grads",
    )(codes_t, err)


def shift(x, axis, k, keep=None):
    size = lax.axis_size(axis)
    pairs = [(i, (i + k) % size) for i in range(size)]
    if keep is not None:
        pairs = [p for p in pairs if keep(*p)]
    return lax.ppermute(x, axis, pairs)


def scatter_sum(x, axis, dim):
    size, me = lax.axis_size(axis), lax.axis_index(axis)
    block = x.shape[dim] // size
    part = lambda i: lax.dynamic_slice_in_dim(x, lax.rem(i, size) * block, block, dim)
    total = part(me)
    for k in range(1, size):
        total = total + shift(part(me + k).astype(jnp.bfloat16), axis, k).astype(jnp.float32)
    return total


def gather_blocks(x, axis, dim):
    size, me = lax.axis_size(axis), lax.axis_index(axis)
    block = x.shape[dim]
    shape = list(x.shape)
    shape[dim] *= size
    out = jnp.zeros(shape, x.dtype)
    for k in range(size):
        piece = x if k == 0 else shift(x, axis, k)
        out = lax.dynamic_update_slice_in_dim(out, piece, lax.rem(me - k + size, size) * block, dim)
    return out


def sum_over(x, axis):
    total = x
    for k in range(1, lax.axis_size(axis)):
        total = total + shift(x, axis, k)
    return total


def on_device(decoder, code_index, code_value, bias, target):
    slab, layers, width = decoder.shape
    tokens, topk = code_index.shape[1:]
    group_count, latent_count = lax.axis_size("grp"), lax.axis_size("latent")
    src, grp, lat_pos = lax.axis_index("src"), lax.axis_index("grp"), lax.axis_index("latent")
    offset = (grp * latent_count + lat_pos) * slab

    index = lax.dynamic_index_in_dim(code_index, src, 0, keepdims=False) - offset
    value = lax.dynamic_index_in_dim(code_value, src, 0, keepdims=False)
    mine = (index >= 0) & (index < slab)
    before = jnp.triu(jnp.ones((topk, topk), jnp.bfloat16), 1)
    rank = jnp.dot(mine.astype(jnp.bfloat16), before, preferred_element_type=jnp.float32).astype(jnp.int32)
    rank = jnp.where(mine, rank, -1)
    counts = jnp.sum(mine.astype(jnp.int32), axis=1)
    groups = jnp.maximum((counts + UNROLL - 1) // UNROLL, 1)
    meta = jnp.stack([jnp.sum(groups), jnp.max(counts)])
    place = rank.T[None] == lax.broadcasted_iota(jnp.int32, (topk, topk, tokens), 0)
    lat = jnp.sum(jnp.where(place, index.T[None], 0), axis=1)
    val = jnp.sum(jnp.where(place, value.astype(jnp.float32).T[None], 0.0), axis=1)

    partial = partial_recon(meta, groups, lat, val, decoder, tokens)

    own = scatter_sum(partial, "grp", 1)
    pick = lambda t: lax.dynamic_index_in_dim(own, jnp.minimum(t, layers - 1), 0, keepdims=False)
    recon = pick(src)
    for k in range(1, layers):
        sent = pick(src + k).astype(jnp.bfloat16)
        recon = recon + shift(sent, "src", k, lambda i, j: i < j).astype(jnp.float32)
    recon = scatter_sum(recon, "latent", 0)
    rows = recon.shape[0]
    start = (grp * latent_count + lat_pos) * rows
    my_target = lax.dynamic_slice(target, (src, start, 0), (1, rows, width))[0]
    my_bias = lax.dynamic_index_in_dim(bias, src, 0, keepdims=True)
    residual = recon + my_bias - my_target.astype(jnp.float32)
    square_sum = jnp.sum(residual * residual)

    mine_err = gather_blocks(residual.astype(jnp.bfloat16), "latent", 0)
    err = jnp.zeros((layers, *mine_err.shape), jnp.bfloat16)
    for k in range(layers):
        piece = mine_err if k == 0 else shift(mine_err, "src", layers - k, lambda i, j: j < i)
        slot = jnp.minimum(src + k, layers - 1)
        old = lax.dynamic_index_in_dim(err, slot, 0, keepdims=False)
        piece = jnp.where(src + k < layers, piece, old)
        err = lax.dynamic_update_index_in_dim(err, piece, slot, 0)
    err = gather_blocks(err, "grp", 1)

    picked = picked_grads(meta, groups, lat, err, decoder)
    picked = jnp.sum(jnp.where(place, picked[:, None, :], 0.0), axis=0)
    packed = jnp.concatenate([picked, jnp.broadcast_to(square_sum, (8, tokens))], axis=0)
    packed = sum_over(sum_over(packed, "grp"), "latent")
    packed = gather_blocks(packed[None], "src", 0)
    code_grad = jnp.swapaxes(packed[:, :topk], 1, 2)
    layer_error = packed[:, topk, 0] / (tokens * width)

    columns = lax.broadcasted_iota(jnp.int32, (slab, tokens), 0)
    codes_t = jnp.zeros((slab, tokens), jnp.float32)
    hits = index.T[:, None, :] == columns[None]
    codes_t = jnp.sum(jnp.where(hits, value.astype(jnp.float32).T[:, None, :], 0.0), axis=0).astype(jnp.bfloat16)
    grads = decoder_grads(codes_t, err, min(128, slab))
    return layer_error, grads, code_grad


def solution(mesh):
    devices = mesh.devices
    layer_count, latent_count = devices.shape
    sources = LAYERS
    fine = Mesh(devices.reshape(sources, layer_count // sources, latent_count), ("src", "grp", "latent"))
    split = P(("src", "grp", "latent"), None, None)
    return jax.shard_map(
        on_device,
        mesh=fine,
        in_specs=(split, P(), P(), P(), P()),
        out_specs=(P(), split, P()),
        check_vma=False,
    )
```
